32 devices in a mesh: ta: 16 (over z, y, x), gz: 2 (over core).
Axes of the slice: x: 2, y: 2, z: 4, core: 2. Of those that a mesh axis runs over, the one named last changes fastest.
Arguments:
- time_links: float32 [2, 3, 3, 32, 8, 256], P(None, None, None, 'ta', 'gz'), may hold values from -1 to 1, as said below
- space_links: float32 [3, 2, 3, 3, 32, 8, 256], P(None, None, None, None, 'ta', 'gz'), may hold values from -1 to 1, as said below
Outputs:
- gauge: float32 [2, 3, 3, 32, 8, 256], P(None, None, None, 'ta', 'gz')
- links_fixed: float32 [3, 2, 3, 3, 32, 8, 256], P(None, None, None, None, 'ta', 'gz')
- action_profile: float32 [32, 8], P('ta', 'gz')
- action_mean: float32 [], replicated
The draws below stay inside these ranges and needn't reach their ends.
Inputs may be any that keep to these rules, and one draw needn't show every extreme that they name: `time_links`: every 3 x 3 complex matrix is unitary up to float32 rounding. `space_links`: every 3 x 3 complex matrix is unitary up to float32 rounding.
All inputs are finite; a program needn't handle non-finite values.
Results may differ from the reference program's by a relative error of at most 0.00024.
Values sent between devices are 32-bit elements; how exact they have to be, the bound alone decides.
A program may use at most 64 MiB of HBM per device.

```python
import jax
import jax.numpy as jnp
from jax import lax

X = 16
Y = 16
NT = 32
NZ = 8


def matrix_product(first_pair, second_pair):
    first_real, first_imag = first_pair
    second_real, second_imag = second_pair
    real_part = jnp.sum(first_real[:, :, None] * second_real[None] - first_imag[:, :, None] * second_imag[None], axis=1)
    imag_part = jnp.sum(first_real[:, :, None] * second_imag[None] + first_imag[:, :, None] * second_real[None], axis=1)
    return (real_part, imag_part)


def embedded_block(first_row, second_row, theta, phi, psi):
    ones = jnp.ones_like(theta)
    zeros = jnp.zeros_like(theta)
    real_rows = [[ones if row == col else zeros for col in range(3)] for row in range(3)]
    imag_rows = [[zeros for col in range(3)] for row in range(3)]
    cosine = jnp.cos(theta)
    sine = jnp.sin(theta)
    real_rows[first_row][first_row] = cosine * jnp.cos(phi)
    imag_rows[first_row][first_row] = cosine * jnp.sin(phi)
    real_rows[first_row][second_row] = sine * jnp.cos(psi)
    imag_rows[first_row][second_row] = sine * jnp.sin(psi)
    real_rows[second_row][first_row] = -sine * jnp.cos(psi)
    imag_rows[second_row][first_row] = sine * jnp.sin(psi)
    real_rows[second_row][second_row] = cosine * jnp.cos(phi)
    imag_rows[second_row][second_row] = -cosine * jnp.sin(phi)
    real_part = jnp.stack([jnp.stack(row_list) for row_list in real_rows])
    imag_part = jnp.stack([jnp.stack(row_list) for row_list in imag_rows])
    return (real_part, imag_part)


def unitary_from_angles(angles):
    result = embedded_block(0, 1, angles[0], angles[1], angles[2])
    result = matrix_product(result, embedded_block(0, 2, angles[3], angles[4], angles[5]))
    result = matrix_product(result, embedded_block(1, 2, angles[6], angles[7], angles[8]))
    return jnp.stack([result[0], result[1]])


def draw_time_links(key, part):
    shape_all = (9, NT, NZ, X * Y)
    angles = 1.5 * jax.random.normal(key, shape_all, jnp.float32)
    return unitary_from_angles(angles)


def draw_space_links(key, part):
    shape_all = (3, 9, NT, NZ, X * Y)
    noise_key = jax.random.fold_in(key, 11)
    slice_key = jax.random.fold_in(key, 23)
    plane_key = jax.random.fold_in(key, 37)
    time_frac = (jnp.arange(NT, dtype=jnp.float32) / max(NT - 1, 1))[:, None, None]
    z_frac = (jnp.arange(NZ, dtype=jnp.float32) / max(NZ - 1, 1))[None, :, None]
    slice_factor = jnp.exp(jax.random.uniform(slice_key, (NT,), jnp.float32, -0.35, 0.35))[:, None, None]
    plane_factor = jnp.exp(jax.random.uniform(plane_key, (NZ,), jnp.float32, -0.2, 0.2))[None, :, None]
    wave = 1.0 + 0.3 * jnp.cos(6.2831853 * 3.0 * time_frac + 0.7)
    noise = jax.random.normal(noise_key, shape_all, jnp.float32)
    rise = (1.0 + z_frac) * jnp.sqrt(1.0 + 0.5 * time_frac)
    amplitude = 0.3 * rise * slice_factor * plane_factor * wave
    directions = []
    for direction in range(3):
        directions.append(unitary_from_angles(amplitude * noise[direction]))
    return jnp.stack(directions)


def setup_inputs(seed: int = 0) -> dict:
    seeds = jax.random.split(jax.random.key(seed), 3)
    return {
        "time_links": draw_time_links(jax.random.fold_in(seeds[2], 71), 0),
        "space_links": draw_space_links(jax.random.fold_in(seeds[2], 71), 0),
    }


def complex_product(first_pair, second_pair):
    first_real, first_imag = first_pair
    second_real, second_imag = second_pair
    real_part = jnp.sum(first_real[:, :, None] * second_real[None] - first_imag[:, :, None] * second_imag[None], axis=1)
    imag_part = jnp.sum(first_real[:, :, None] * second_imag[None] + first_imag[:, :, None] * second_real[None], axis=1)
    return real_part, imag_part


def dagger(matrix_pair):
    return jnp.swapaxes(matrix_pair[0], 0, 1), -jnp.swapaxes(matrix_pair[1], 0, 1)


def plane_step(matrix_pair, direction):
    def shifted(values):
        leading = values.shape[:-1]
        lattice_grid = values.reshape(leading + (X, Y))
        lattice_grid = jnp.roll(lattice_grid, -1, axis=lattice_grid.ndim - 2 + direction)
        return lattice_grid.reshape(leading + (X * Y,))
    return shifted(matrix_pair[0]), shifted(matrix_pair[1])


def roll_upward(matrix_pair):
    return jnp.roll(matrix_pair[0], -1, axis=-2), jnp.roll(matrix_pair[1], -1, axis=-2)


def plaquette_density(link_set, forward_x, forward_y):
    forward_z = [forward_x, forward_y]
    terms = []
    for first_dir, second_dir in ((0, 1), (0, 2), (1, 2)):
        along_first = link_set[first_dir]
        along_second = link_set[second_dir]
        second_moved = plane_step(along_second, first_dir)
        if second_dir < 2:
            first_moved = plane_step(along_first, second_dir)
        else:
            first_moved = forward_z[first_dir]
        loop_matrix = complex_product(complex_product(along_first, second_moved),
                                      complex_product(dagger(first_moved), dagger(along_second)))
        trace_real = loop_matrix[0][0, 0] + loop_matrix[0][1, 1] + loop_matrix[0][2, 2]
        terms.append(1.0 - trace_real / 3.0)
    return terms[0] + terms[1] + terms[2]


def reference(time_links, space_links):
    unit_real = jnp.broadcast_to(jnp.eye(3, dtype=jnp.float32)[:, :, None, None], (3, 3, NZ, X * Y))
    start_pair = (unit_real, jnp.zeros_like(unit_real))

    def advance(carry_pair, link_block):
        return complex_product(carry_pair, (link_block[0], link_block[1])), jnp.stack(carry_pair)

    unused_final, gauge_steps = lax.scan(advance, start_pair, jnp.moveaxis(time_links, 3, 0))
    gauge = jnp.moveaxis(gauge_steps, 0, 3)
    gauge_pair = (gauge[0], gauge[1])
    fixed = []
    for direction in range(3):
        link_pair = (space_links[direction, 0], space_links[direction, 1])
        if direction < 2:
            ahead = plane_step(gauge_pair, direction)
        else:
            ahead = roll_upward(gauge_pair)
        fixed.append(complex_product(complex_product(gauge_pair, link_pair), dagger(ahead)))
    links_fixed = jnp.stack([jnp.stack(pair) for pair in fixed])
    density = plaquette_density(fixed, roll_upward(fixed[0]), roll_upward(fixed[1]))
    action_profile = jnp.mean(density, axis=-1) / 3.0
    action_mean = jnp.mean(action_profile)
    return gauge, links_fixed, action_profile, action_mean
```

```python
import functools

import jax
import jax.numpy as jnp
from jax import lax
from jax.experimental import pallas as pl
from jax.experimental.pallas import tpu as pltpu
from jax.sharding import PartitionSpec as P

X = 16
Y = 16
LANES = 128
MESH = pl.DeviceIdType.MESH
PACK = 16


def to_rows(a):
    lead, (z, s), n = a.shape[:-2], a.shape[-2:], a.ndim - 2
    a = jnp.swapaxes(a.reshape(lead + (z, s // LANES, LANES)), n, n + 1)
    return a.reshape(lead + (z * (s // LANES), LANES))


def from_rows(a, z, s):
    lead, n = a.shape[:-2], a.ndim - 2
    a = jnp.swapaxes(a.reshape(lead + (s // LANES, z, LANES)), n, n + 1)
    return a.reshape(lead + (z, s))


def product(a, b, rows=(0, 1, 2)):
    re, im = {}, {}
    for i in rows:
        for j in range(3):
            r = m = None
            for k in range(3):
                rr = a[0][i, k] * b[0][k, j] - a[1][i, k] * b[1][k, j]
                mm = a[0][i, k] * b[1][k, j] + a[1][i, k] * b[0][k, j]
                r = rr if r is None else r + rr
                m = mm if m is None else m + mm
            re[i, j], im[i, j] = r, m
    return re, im


def product_dagger(a, b):
    re, im = {}, {}
    for i in range(3):
        for j in range(3):
            r = m = None
            for k in range(3):
                rr = a[0][i, k] * b[0][j, k] + a[1][i, k] * b[1][j, k]
                mm = a[1][i, k] * b[0][j, k] - a[0][i, k] * b[1][j, k]
                r = rr if r is None else r + rr
                m = mm if m is None else m + mm
            re[i, j], im[i, j] = r, m
    return re, im


def cross_conj(m):
    re, im = m
    out_re, out_im = [], []
    for j in range(3):
        p, q = (j + 1) % 3, (j + 2) % 3
        out_re.append(
            (re[0, p] * re[1, q] - im[0, p] * im[1, q])
            - (re[0, q] * re[1, p] - im[0, q] * im[1, p])
        )
        out_im.append(
            (re[0, q] * im[1, p] + im[0, q] * re[1, p])
            - (re[0, p] * im[1, q] + im[0, p] * re[1, q])
        )
    return out_re, out_im


def determinant(m):
    wr, wi = cross_conj(m)
    re, im = m
    dr = sum(wr[j] * re[2, j] + wi[j] * im[2, j] for j in range(3))
    di = sum(wr[j] * im[2, j] - wi[j] * re[2, j] for j in range(3))
    return dr, di


def with_last_row(top, det):
    wr, wi = cross_conj(top)
    re, im = dict(top[0]), dict(top[1])
    for j in range(3):
        re[2, j] = det[0] * wr[j] - det[1] * wi[j]
        im[2, j] = det[0] * wi[j] + det[1] * wr[j]
    return re, im


TOP = [(i, j) for i in range(2) for j in range(3)]


def packed(top, det):
    return [top[0][e] for e in TOP] + [top[1][e] for e in TOP] + list(det)


def unpacked(v):
    top = ({e: v[n] for n, e in enumerate(TOP)}, {e: v[6 + n] for n, e in enumerate(TOP)})
    return top, (v[12], v[13])


def det_product(a, b):
    return a[0] * b[0] - a[1] * b[1], a[0] * b[1] + a[1] * b[0]


def put(ref, lead, count, values):
    for k, v in enumerate(values):
        ref[lead + (pl.ds(k, count, stride=PACK), slice(None))] = v


def get(ref, lead, count):
    return unpacked(
        [ref[lead + (pl.ds(k, count, stride=PACK), slice(None))] for k in range(14)]
    )


def kernel(
    sizes,
    time_in, space_in, gauge_out, fixed_out, profile_out, mean_out,
    tb, sb, gb, fb, halo_s, halo_g, pbuf, buf1, tot, buf2, obuf, gbuf, msg, m1, m2, m3,
    in_sem, out_sem, s1, r1, s2, r2, s3, r3, hs_sem, hg_sem, ms1, mr1, ms2, mr2, ms3, mr3,
):
    steps, layers, n_gz, n_lo, n_hi = sizes
    rows = tb.shape[-2]
    part = rows // n_lo
    size = part * PACK
    ta, gz = lax.axis_index("ta"), lax.axis_index("gz")
    hi, lo = ta // n_lo, ta % n_lo

    load_t = pltpu.make_async_copy(time_in, tb, in_sem.at[0])
    load_t.start()
    load_s = pltpu.make_async_copy(space_in, sb, in_sem.at[1])
    load_s.start()

    def lo_at(d):
        return hi * n_lo + (lo + d) % n_lo

    def gz_at(d):
        return (gz + d) % n_gz

    def hi_at(d):
        return ((hi + d) % n_hi) * n_lo + lo

    barrier = pltpu.get_barrier_semaphore()
    for d in range(1, n_gz):
        pl.semaphore_signal(barrier, inc=1, device_id=(ta, gz_at(d)), device_id_type=MESH)
    for d in range(1, n_lo):
        pl.semaphore_signal(barrier, inc=1, device_id=(lo_at(d), gz), device_id_type=MESH)
    for d in range(1, n_hi):
        pl.semaphore_signal(barrier, inc=1, device_id=(hi_at(d), gz), device_id_type=MESH)

    def matrix(ref, lead, t):
        re = {(i, j): ref[lead + (0, i, j, t)] for i in range(3) for j in range(3)}
        im = {(i, j): ref[lead + (1, i, j, t)] for i in range(3) for j in range(3)}
        return re, im

    def remote(src, dst, send, recv, device):
        return pltpu.make_async_remote_copy(
            src_ref=src, dst_ref=dst, send_sem=send, recv_sem=recv,
            device_id=device, device_id_type=MESH,
        )

    lane = lax.broadcasted_iota(jnp.int32, (rows, LANES), 1)
    row = lax.broadcasted_iota(jnp.int32, (rows, LANES), 0)
    last_x = lane >= LANES - Y
    last_y = lane % Y == Y - 1
    last_z = row % layers == layers - 1

    def step_x(v):
        r = pltpu.roll(v, LANES - Y, 1)
        return jnp.where(last_x, pltpu.roll(r, rows - layers, 0), r)

    def step_y(v):
        return jnp.where(last_y, pltpu.roll(v, Y - 1, 1), pltpu.roll(v, LANES - 1, 1))

    def step_z(v, upper):
        return jnp.where(last_z, pltpu.roll(upper, layers - 1, 0), pltpu.roll(v, rows - 1, 0))

    def moved(f, *ms):
        return tuple({e: f(*(m[c][e] for m in ms)) for e in ms[0][c]} for c in range(2))

    load_t.wait()
    local = matrix(tb, (), 0)
    for t in range(1, steps):
        local = product(local, matrix(tb, (), t))
    put(pbuf, (), rows, packed(local, determinant(local)))

    pl.semaphore_wait(barrier, n_gz - 1 + n_lo - 1 + n_hi - 1)

    def mine(d):
        return pl.ds(pl.multiple_of(((lo + d) % n_lo) * size, 8), size)

    first = [pltpu.make_async_copy(pbuf.at[mine(0)], buf1.at[lo], s1.at[0])]
    for d in range(1, n_lo):
        first.append(remote(pbuf.at[mine(d)], buf1.at[lo], s1.at[d], r1.at[d], (lo_at(d), gz)))
    for c in first[1:] + first[:1]:
        c.start()
    load_s.wait()
    halo_link = remote(
        sb.at[pl.ds(0, 2)], halo_s, hs_sem.at[0], hs_sem.at[1], (ta, gz_at(n_gz - 1))
    )
    halo_link.start()

    def plaquette(a, b_moved, a_moved, b):
        u, v = product(a, b_moved), product(b, a_moved)
        re = sum(u[0][e] * v[0][e] + u[1][e] * v[1][e] for e in u[0])
        return 1.0 - re / 3.0

    density = []
    for t in range(steps):
        x, y = matrix(sb, (0,), t), matrix(sb, (1,), t)
        density.append(plaquette(x, moved(step_x, y), moved(step_y, x), y))
    halo_link.wait_recv()
    for t in range(steps):
        z = matrix(sb, (2,), t)
        for mu, step in ((0, step_x), (1, step_y)):
            a = matrix(sb, (mu,), t)
            up = moved(step_z, a, matrix(halo_s, (mu,), t))
            density[t] = density[t] + plaquette(a, moved(step, z), up, z)
    sites = rows // layers * LANES
    total = None
    for t in range(steps):
        per_row = jnp.broadcast_to(jnp.sum(density[t], axis=1, keepdims=True), (rows, LANES))
        spread = jnp.where(row % layers == lane, per_row, 0.0)
        line = jnp.sum(spread, axis=0, keepdims=True)
        profile_out[t : t + 1, :] = line[:, :layers] / float(sites) / 3.0
        total = per_row if total is None else total + per_row
    total = jnp.broadcast_to(jnp.sum(total, axis=0, keepdims=True), (rows, LANES))

    def spread_sum(n, stage, buf, me, send, recv, device):
        buf[me] = total_at[0]
        msg[stage] = total_at[0]
        out = [
            remote(msg.at[stage], buf.at[me], send.at[d], recv.at[d], device(d))
            for d in range(1, n)
        ]
        for c in out:
            c.start()
        return out

    def gather_sum(n, stage, buf, me, send, recv, device):
        for d in range(1, n):
            remote(
                msg.at[stage], buf.at[(me + n - d) % n], send.at[d], recv.at[d], device(d)
            ).wait_recv()
        got = buf[0]
        for k in range(1, n):
            got = got + buf[k]
        total_at[0] = got

    total_at = [total]
    stage1 = (n_gz, 0, m1, gz, ms1, mr1, lambda d: (ta, gz_at(d)))
    stage2 = (n_lo, 1, m2, lo, ms2, mr2, lambda d: (lo_at(d), gz))
    stage3 = (n_hi, 2, m3, hi, ms3, mr3, lambda d: (hi_at(d), gz))
    sent = spread_sum(*stage1)

    first[0].wait()
    for d in range(1, n_lo):
        remote(
            pbuf.at[mine(d)], buf1.at[(lo + n_lo - d) % n_lo], s1.at[d], r1.at[d], (lo_at(d), gz)
        ).wait_recv()
    before = [None]
    run, run_det = get(buf1, (0,), part)
    for k in range(1, n_lo):
        before.append((run, run_det))
        nxt, nxt_det = get(buf1, (k,), part)
        run = product(run, with_last_row(nxt, nxt_det), rows=(0, 1))
        run_det = det_product(run_det, nxt_det)
    put(tot, (), part, packed(run, run_det))

    def second(d, slot):
        return remote(tot, buf2.at[slot], s2.at[d], r2.at[d], (hi_at(d), gz))

    for d in range(1, n_hi):
        pl.when(hi + d < n_hi)(second(d, hi).start)
    gather_sum(*stage1)
    sent += spread_sum(*stage2)
    gather_sum(*stage2)
    sent += spread_sum(*stage3)
    full_before = [None] + [with_last_row(*b) for b in before[1:]]
    for d in range(1, n_hi):
        pl.when(hi >= d)(second(d, (hi + n_hi - d) % n_hi).wait_recv)

    zero = jnp.zeros((part, LANES), jnp.float32)
    one = jnp.ones((part, LANES), jnp.float32)
    acc = ({e: one if e[0] == e[1] else zero for e in TOP}, {e: zero for e in TOP})
    acc_det = (one, zero)
    for k in range(n_hi - 1):
        nxt, nxt_det = get(buf2, (k,), part)
        if k == 0:
            new, new_det = nxt, nxt_det
        else:
            new = product(acc, with_last_row(nxt, nxt_det), rows=(0, 1))
            new_det = det_product(acc_det, nxt_det)
        use = k < hi
        acc = moved(lambda n, o: jnp.where(use, n, o), new, acc)
        acc_det = tuple(jnp.where(use, n, o) for n, o in zip(new_det, acc_det))

    put(obuf, (0,), part, packed(acc, acc_det))
    for k in range(1, n_lo):
        top = product(acc, full_before[k], rows=(0, 1))
        put(obuf, (k,), part, packed(top, det_product(acc_det, before[k][1])))
    third = [pltpu.make_async_copy(obuf.at[lo], gbuf.at[mine(0)], s3.at[0])]
    for d in range(1, n_lo):
        third.append(
            remote(obuf.at[(lo + d) % n_lo], gbuf.at[mine(0)], s3.at[d], r3.at[d], (lo_at(d), gz))
        )
    for c in third[1:] + third[:1]:
        c.start()
    third[0].wait()
    for d in range(1, n_lo):
        remote(
            obuf.at[(lo + d) % n_lo], gbuf.at[mine(n_lo - d)], s3.at[d], r3.at[d], (lo_at(d), gz)
        ).wait_recv()

    def keep(ref, lead, t, m):
        for i in range(3):
            for j in range(3):
                ref[lead + (0, i, j, t)] = m[0][i, j]
                ref[lead + (1, i, j, t)] = m[1][i, j]

    gauge = with_last_row(*get(gbuf, (), rows))
    for t in range(steps):
        keep(gb, (), t, gauge)
        if t < steps - 1:
            gauge = product(gauge, matrix(tb, (), t))
    halo_gauge = remote(gb, halo_g, hg_sem.at[0], hg_sem.at[1], (ta, gz_at(n_gz - 1)))
    halo_gauge.start()
    stores = [pltpu.make_async_copy(gb, gauge_out, out_sem.at[0])]
    stores[0].start()

    for mu in range(3):
        if mu == 2:
            halo_gauge.wait_recv()
        for t in range(steps):
            g = matrix(gb, (), t)
            if mu == 2:
                ahead = moved(step_z, g, matrix(halo_g, (), t))
            else:
                ahead = moved((step_x, step_y)[mu], g)
            keep(fb, (mu,), t, product_dagger(product(g, matrix(sb, (mu,), t)), ahead))
        stores.append(pltpu.make_async_copy(fb.at[mu], fixed_out.at[mu], out_sem.at[1 + mu]))
        stores[-1].start()

    gather_sum(*stage3)
    count = sites * 3.0 * steps * layers * n_gz * n_lo * n_hi
    mean_out[...] = total_at[0][0:1, 0:1] / count

    for c in first[1:] + third[1:] + sent + [halo_link, halo_gauge]:
        c.wait_send()
    for d in range(1, n_hi):
        pl.when(hi + d < n_hi)(second(d, hi).wait_send)
    for c in stores:
        c.wait()


def on_device(n_ta, n_gz, time_links, space_links):
    steps, layers, sites = time_links.shape[3:]
    n_lo = 1
    while n_lo * 2 * n_lo * 2 <= n_ta:
        n_lo *= 2
    n_hi = n_ta // n_lo
    t_rows, s_rows = to_rows(time_links), to_rows(space_links)
    rows = t_rows.shape[-2]
    size = rows // n_lo * PACK
    f32 = jnp.float32
    dma = pltpu.SemaphoreType.DMA
    anywhere = pl.BlockSpec(memory_space=pl.ANY)
    vmem = pl.BlockSpec(memory_space=pltpu.VMEM)
    gauge, fixed, profile, mean = pl.pallas_call(
        functools.partial(kernel, (steps, layers, n_gz, n_lo, n_hi)),
        out_shape=[
            jax.ShapeDtypeStruct(t_rows.shape, f32),
            jax.ShapeDtypeStruct(s_rows.shape, f32),
            jax.ShapeDtypeStruct((steps, layers), f32),
            jax.ShapeDtypeStruct((1, 1), f32),
        ],
        in_specs=[anywhere, anywhere],
        out_specs=[anywhere, anywhere, vmem, vmem],
        scratch_shapes=[
            pltpu.VMEM(t_rows.shape, f32),
            pltpu.VMEM(s_rows.shape, f32),
            pltpu.VMEM(t_rows.shape, f32),
            pltpu.VMEM(s_rows.shape, f32),
            pltpu.VMEM((2,) + s_rows.shape[1:], f32),
            pltpu.VMEM(t_rows.shape, f32),
            pltpu.VMEM((rows * PACK, LANES), f32),
            pltpu.VMEM((n_lo, size, LANES), f32),
            pltpu.VMEM((size, LANES), f32),
            pltpu.VMEM((n_hi, size, LANES), f32),
            pltpu.VMEM((n_lo, size, LANES), f32),
            pltpu.VMEM((rows * PACK, LANES), f32),
            pltpu.VMEM((3, rows, LANES), f32),
            pltpu.VMEM((n_gz, rows, LANES), f32),
            pltpu.VMEM((n_lo, rows, LANES), f32),
            pltpu.VMEM((n_hi, rows, LANES), f32),
            dma((2,)), dma((4,)),
            dma((n_lo,)), dma((n_lo,)), dma((n_hi,)), dma((n_hi,)), dma((n_lo,)), dma((n_lo,)),
            dma((2,)), dma((2,)),
            dma((n_gz,)), dma((n_gz,)), dma((n_lo,)), dma((n_lo,)), dma((n_hi,)), dma((n_hi,)),
        ],
        compiler_params=pltpu.CompilerParams(collective_id=0, has_side_effects=True),
    )(t_rows, s_rows)
    return (
        from_rows(gauge, layers, sites),
        from_rows(fixed, layers, sites),
        profile,
        mean.reshape(()),
    )


def solution(mesh):
    return jax.shard_map(
        functools.partial(on_device, mesh.shape["ta"], mesh.shape["gz"]),
        mesh=mesh,
        in_specs=(
            P(None, None, None, "ta", "gz", None),
            P(None, None, None, None, "ta", "gz", None),
        ),
        out_specs=(
            P(None, None, None, "ta", "gz", None),
            P(None, None, None, None, "ta", "gz", None),
            P("ta", "gz"),
            P(),
        ),
        check_vma=False,
    )
```

```python
import functools

import jax
import jax.numpy as jnp
from jax import lax
from jax.experimental import pallas as pl
from jax.experimental.pallas import tpu as pltpu
from jax.sharding import PartitionSpec as P

X = 16
Y = 16
LANES = 128
GRANT = 8 << 20
MESH = pl.DeviceIdType.MESH
PACK = 16


def to_rows(a):
    lead, (z, s), n = a.shape[:-2], a.shape[-2:], a.ndim - 2
    a = jnp.swapaxes(a.reshape(lead + (z, s // LANES, LANES)), n, n + 1)
    return a.reshape(lead + (z * (s // LANES), LANES))


def from_rows(a, z, s):
    lead, n = a.shape[:-2], a.ndim - 2
    a = jnp.swapaxes(a.reshape(lead + (s // LANES, z, LANES)), n, n + 1)
    return a.reshape(lead + (z, s))


def product(a, b, rows=(0, 1, 2)):
    re, im = {}, {}
    for i in rows:
        for j in range(3):
            r = m = None
            for k in range(3):
                rr = a[0][i, k] * b[0][k, j] - a[1][i, k] * b[1][k, j]
                mm = a[0][i, k] * b[1][k, j] + a[1][i, k] * b[0][k, j]
                r = rr if r is None else r + rr
                m = mm if m is None else m + mm
            re[i, j], im[i, j] = r, m
    return re, im


def product_dagger(a, b):
    re, im = {}, {}
    for i in range(3):
        for j in range(3):
            r = m = None
            for k in range(3):
                rr = a[0][i, k] * b[0][j, k] + a[1][i, k] * b[1][j, k]
                mm = a[1][i, k] * b[0][j, k] - a[0][i, k] * b[1][j, k]
                r = rr if r is None else r + rr
                m = mm if m is None else m + mm
            re[i, j], im[i, j] = r, m
    return re, im


def cross_conj(m):
    re, im = m
    out_re, out_im = [], []
    for j in range(3):
        p, q = (j + 1) % 3, (j + 2) % 3
        out_re.append(
            (re[0, p] * re[1, q] - im[0, p] * im[1, q])
            - (re[0, q] * re[1, p] - im[0, q] * im[1, p])
        )
        out_im.append(
            (re[0, q] * im[1, p] + im[0, q] * re[1, p])
            - (re[0, p] * im[1, q] + im[0, p] * re[1, q])
        )
    return out_re, out_im


def determinant(m):
    wr, wi = cross_conj(m)
    re, im = m
    dr = sum(wr[j] * re[2, j] + wi[j] * im[2, j] for j in range(3))
    di = sum(wr[j] * im[2, j] - wi[j] * re[2, j] for j in range(3))
    return dr, di


def with_last_row(top, det):
    wr, wi = cross_conj(top)
    re, im = dict(top[0]), dict(top[1])
    for j in range(3):
        re[2, j] = det[0] * wr[j] - det[1] * wi[j]
        im[2, j] = det[0] * wi[j] + det[1] * wr[j]
    return re, im


TOP = [(i, j) for i in range(2) for j in range(3)]


def packed(top, det):
    return [top[0][e] for e in TOP] + [top[1][e] for e in TOP] + list(det)


def unpacked(v):
    top = ({e: v[n] for n, e in enumerate(TOP)}, {e: v[6 + n] for n, e in enumerate(TOP)})
    return top, (v[12], v[13])


def det_product(a, b):
    return a[0] * b[0] - a[1] * b[1], a[0] * b[1] + a[1] * b[0]


def put(ref, lead, count, values):
    for k, v in enumerate(values):
        ref[lead + (pl.ds(k, count, stride=PACK), slice(None))] = v


def get(ref, lead, count):
    return unpacked(
        [ref[lead + (pl.ds(k, count, stride=PACK), slice(None))] for k in range(14)]
    )


def matrix(ref, lead, t):
    re = {(i, j): ref[lead + (0, i, j, t)] for i in range(3) for j in range(3)}
    im = {(i, j): ref[lead + (1, i, j, t)] for i in range(3) for j in range(3)}
    return re, im


def keep(ref, lead, t, m):
    for i in range(3):
        for j in range(3):
            ref[lead + (0, i, j, t)] = m[0][i, j]
            ref[lead + (1, i, j, t)] = m[1][i, j]


def moved(f, *ms):
    return tuple({e: f(*(m[c][e] for m in ms)) for e in ms[0][c]} for c in range(2))


def steppers(rows, layers):
    lane = lax.broadcasted_iota(jnp.int32, (rows, LANES), 1)
    row = lax.broadcasted_iota(jnp.int32, (rows, LANES), 0)
    last_x = lane >= LANES - Y
    last_y = lane % Y == Y - 1
    last_z = row % layers == layers - 1

    def step_x(v):
        r = pltpu.roll(v, LANES - Y, 1)
        return jnp.where(last_x, pltpu.roll(r, rows - layers, 0), r)

    def step_y(v):
        return jnp.where(last_y, pltpu.roll(v, Y - 1, 1), pltpu.roll(v, LANES - 1, 1))

    def step_z(v, upper):
        return jnp.where(last_z, pltpu.roll(upper, layers - 1, 0), pltpu.roll(v, rows - 1, 0))

    return step_x, step_y, step_z, lane, row


def scan_kernel(
    sizes,
    time_in, space_in, gauge_out, above_out, profile_out, mean_out, tb, sb,
    halo_t, halo_s, pbuf, buf1, tot, buf2, obuf, gbuf, hbuf, msg, m1, m2, m3,
    in_sem, s1, r1, s2, r2, s3, r3, s4, r4, hs_sem, ht_sem, ms1, mr1, ms2, mr2, ms3, mr3,
):
    steps, layers, n_gz, n_lo, n_hi = sizes
    rows = tb.shape[-2]
    part = rows // n_lo
    size = part * PACK
    ta, gz = lax.axis_index("ta"), lax.axis_index("gz")
    hi, lo = ta // n_lo, ta % n_lo

    load_t = pltpu.make_async_copy(time_in, tb, in_sem.at[0])
    load_t.start()
    load_s = pltpu.make_async_copy(space_in, sb, in_sem.at[1])
    load_s.start()

    def flip(m):
        out, bit = 0, 1
        while bit < n_lo:
            b = (lo // bit) % 2
            out = out + bit * (1 - b if m & bit else b)
            bit *= 2
        return out

    def lo_at(m):
        return hi * n_lo + flip(m)

    def gz_at(d):
        return (gz + d) % n_gz

    def hi_at(d):
        return ((hi + d) % n_hi) * n_lo + lo

    barrier = pltpu.get_barrier_semaphore()
    for d in range(1, n_gz):
        pl.semaphore_signal(barrier, inc=1, device_id=(ta, gz_at(d)), device_id_type=MESH)
    for d in range(1, n_lo):
        pl.semaphore_signal(barrier, inc=1, device_id=(lo_at(d), gz), device_id_type=MESH)
    for d in range(1, n_hi):
        pl.semaphore_signal(barrier, inc=1, device_id=(hi_at(d), gz), device_id_type=MESH)
    near = sorted({1, n_gz - 1})
    for g in near:
        for d in range(1, n_lo):
            pl.semaphore_signal(
                barrier, inc=1, device_id=(lo_at(d), gz_at(g)), device_id_type=MESH
            )

    def remote(src, dst, send, recv, device):
        return pltpu.make_async_remote_copy(
            src_ref=src, dst_ref=dst, send_sem=send, recv_sem=recv,
            device_id=device, device_id_type=MESH,
        )

    step_x, step_y, step_z, lane, row = steppers(rows, layers)

    load_t.wait()
    local = matrix(tb, (), 0)
    for t in range(1, steps):
        local = product(local, matrix(tb, (), t))
    put(pbuf, (), rows, packed(local, determinant(local)))

    pl.semaphore_wait(barrier, n_gz - 1 + (n_lo - 1) * (1 + len(near)) + n_hi - 1)

    def mine(d):
        return pl.ds(pl.multiple_of(flip(d) * size, 8), size)

    far_first = sorted(range(1, n_lo), key=lambda m: -bin(m).count("1"))
    first = [pltpu.make_async_copy(pbuf.at[mine(0)], buf1.at[lo], s1.at[0])]
    for d in far_first:
        first.append(remote(pbuf.at[mine(d)], buf1.at[lo], s1.at[d], r1.at[d], (lo_at(d), gz)))
    for c in first[1:] + first[:1]:
        c.start()
    load_s.wait()
    below = gz_at(n_gz - 1)
    halo_link = remote(sb.at[pl.ds(0, 2)], halo_s, hs_sem.at[0], hs_sem.at[1], (ta, below))
    halo_link.start()
    halo_time = remote(
        tb.at[:, :, :, pl.ds(0, steps - 1)], halo_t, ht_sem.at[0], ht_sem.at[1], (ta, below)
    )
    if steps > 1:
        halo_time.start()

    def plaquette(a, b_moved, a_moved, b):
        u, v = product(a, b_moved), product(b, a_moved)
        re = sum(u[0][e] * v[0][e] + u[1][e] * v[1][e] for e in u[0])
        return 1.0 - re / 3.0

    density = []
    for t in range(steps):
        x, y = matrix(sb, (0,), t), matrix(sb, (1,), t)
        density.append(plaquette(x, moved(step_x, y), moved(step_y, x), y))
    halo_link.wait_recv()
    for t in range(steps):
        z = matrix(sb, (2,), t)
        for mu, step in ((0, step_x), (1, step_y)):
            a = matrix(sb, (mu,), t)
            up = moved(step_z, a, matrix(halo_s, (mu,), t))
            density[t] = density[t] + plaquette(a, moved(step, z), up, z)
    sites = rows // layers * LANES
    total = None
    for t in range(steps):
        per_row = jnp.broadcast_to(jnp.sum(density[t], axis=1, keepdims=True), (rows, LANES))
        spread = jnp.where(row % layers == lane, per_row, 0.0)
        line = jnp.sum(spread, axis=0, keepdims=True)
        profile_out[t : t + 1, :] = line[:, :layers] / float(sites) / 3.0
        total = per_row if total is None else total + per_row
    total = jnp.broadcast_to(jnp.sum(total, axis=0, keepdims=True), (rows, LANES))

    def spread_sum(n, stage, buf, me, send, recv, device, source):
        buf[me] = total_at[0]
        msg[stage] = total_at[0]
        out = [
            remote(msg.at[stage], buf.at[me], send.at[d], recv.at[d], device(d))
            for d in range(1, n)
        ]
        for c in out:
            c.start()
        return out

    def gather_sum(n, stage, buf, me, send, recv, device, source):
        for d in range(1, n):
            remote(
                msg.at[stage], buf.at[source(d)], send.at[d], recv.at[d], device(d)
            ).wait_recv()
        got = buf[0]
        for k in range(1, n):
            got = got + buf[k]
        total_at[0] = got

    total_at = [total]
    stage1 = (n_gz, 0, m1, gz, ms1, mr1, lambda d: (ta, gz_at(d)), lambda d: gz_at(n_gz - d))
    stage2 = (n_lo, 1, m2, lo, ms2, mr2, lambda d: (lo_at(d), gz), flip)
    stage3 = (n_hi, 2, m3, hi, ms3, mr3, lambda d: (hi_at(d), gz), lambda d: (hi + n_hi - d) % n_hi)
    sent = spread_sum(*stage1)

    first[0].wait()
    for d in range(1, n_lo):
        remote(
            pbuf.at[mine(d)], buf1.at[flip(d)], s1.at[d], r1.at[d], (lo_at(d), gz)
        ).wait_recv()
    before = [None]
    run, run_det = get(buf1, (0,), part)
    for k in range(1, n_lo):
        before.append((run, run_det))
        nxt, nxt_det = get(buf1, (k,), part)
        run = product(run, with_last_row(nxt, nxt_det), rows=(0, 1))
        run_det = det_product(run_det, nxt_det)
    put(tot, (), part, packed(run, run_det))

    def second(d, slot):
        return remote(tot, buf2.at[slot], s2.at[d], r2.at[d], (hi_at(d), gz))

    for d in reversed(range(1, n_hi)):
        pl.when(hi + d < n_hi)(second(d, hi).start)
    gather_sum(*stage1)
    sent += spread_sum(*stage2)
    gather_sum(*stage2)
    sent += spread_sum(*stage3)
    full_before = [None] + [with_last_row(*b) for b in before[1:]]
    for d in range(1, n_hi):
        pl.when(hi >= d)(second(d, (hi + n_hi - d) % n_hi).wait_recv)

    zero = jnp.zeros((part, LANES), jnp.float32)
    one = jnp.ones((part, LANES), jnp.float32)
    acc = ({e: one if e[0] == e[1] else zero for e in TOP}, {e: zero for e in TOP})
    acc_det = (one, zero)
    for k in range(n_hi - 1):
        nxt, nxt_det = get(buf2, (k,), part)
        if k == 0:
            new, new_det = nxt, nxt_det
        else:
            new = product(acc, with_last_row(nxt, nxt_det), rows=(0, 1))
            new_det = det_product(acc_det, nxt_det)
        use = k < hi
        acc = moved(lambda n, o: jnp.where(use, n, o), new, acc)
        acc_det = tuple(jnp.where(use, n, o) for n, o in zip(new_det, acc_det))

    put(obuf, (0,), part, packed(acc, acc_det))
    for k in range(1, n_lo):
        top = product(acc, full_before[k], rows=(0, 1))
        put(obuf, (k,), part, packed(top, det_product(acc_det, before[k][1])))
    third = [pltpu.make_async_copy(obuf.at[lo], gbuf.at[mine(0)], s3.at[0])]
    for d in far_first:
        third.append(
            remote(obuf.at[flip(d)], gbuf.at[mine(0)], s3.at[d], r3.at[d], (lo_at(d), gz))
        )
    lowest = (lo * part) % layers == 0

    def fourth(d, source):
        rows_there = pl.ds(pl.multiple_of(source * size, 8), PACK)
        return remote(
            obuf.at[flip(d), pl.ds(0, PACK)], hbuf.at[rows_there], s4.at[d], r4.at[source],
            (lo_at(d), below),
        )

    for c in third[1:]:
        c.start()
    for d in far_first + [0]:
        pl.when(lowest)(fourth(d, lo).start)
    third[0].start()
    if steps > 1:
        halo_time.wait_recv()
    gather_sum(*stage3)
    count = sites * 3.0 * steps * layers * n_gz * n_lo * n_hi
    mean_out[...] = total_at[0] / count
    third[0].wait()
    for d in range(1, n_lo):
        remote(
            obuf.at[flip(d)], gbuf.at[mine(d)], s3.at[d], r3.at[d], (lo_at(d), gz)
        ).wait_recv()
    for k in range(14):
        gauge_out[k] = gbuf[pl.ds(k, rows, stride=PACK), :]
    for k in range(n_lo):
        if (k * part) % layers == 0:
            fourth(0, k).wait_recv()
    above = with_last_row(*get(hbuf, (), rows))
    for t in range(steps):
        keep(above_out, (), t, above)
        if t < steps - 1:
            above = product(above, matrix(halo_t, (), t))

    for c in first[1:] + third[1:] + sent + [halo_link]:
        c.wait_send()
    if steps > 1:
        halo_time.wait_send()
    for d in range(n_lo):
        pl.when(lowest)(fourth(d, lo).wait_send)
    for d in range(1, n_hi):
        pl.when(hi + d < n_hi)(second(d, hi).wait_send)


def fix_kernel(
    sizes,
    packed_in, above_in, profile_in, mean_in, tb, sb,
    gauge_out, fixed_out, profile_out, mean_out,
    gb, fb, pb, mb, out_sem,
):
    steps, layers = sizes
    rows = tb.shape[-2]
    pb[...] = profile_in[...]
    mb[...] = mean_in[0:1, 0:1]
    stores = [
        pltpu.make_async_copy(pb, profile_out, out_sem.at[4]),
        pltpu.make_async_copy(mb, mean_out, out_sem.at[5]),
    ]
    for c in stores:
        c.start()
    step_x, step_y, step_z, _, _ = steppers(rows, layers)
    gauge = with_last_row(*unpacked([packed_in[k] for k in range(14)]))
    for t in range(steps):
        keep(gb, (), t, gauge)
        if t < steps - 1:
            gauge = product(gauge, matrix(tb, (), t))
    stores.append(pltpu.make_async_copy(gb, gauge_out, out_sem.at[3]))
    stores[-1].start()
    for mu in range(3):
        for t in range(steps):
            g = matrix(gb, (), t)
            if mu == 2:
                ahead = moved(step_z, g, matrix(above_in, (), t))
            else:
                ahead = moved((step_x, step_y)[mu], g)
            keep(fb, (mu,), t, product_dagger(product(g, matrix(sb, (mu,), t)), ahead))
        stores.append(pltpu.make_async_copy(fb.at[mu], fixed_out.at[mu], out_sem.at[mu]))
        stores[-1].start()
    for c in stores:
        c.wait()


def on_device(n_ta, n_gz, time_links, space_links):
    steps, layers, sites = time_links.shape[3:]
    n_lo = 1
    while n_lo * 2 * n_lo * 2 <= n_ta:
        n_lo *= 2
    n_hi = n_ta // n_lo
    t_rows, s_rows = to_rows(time_links), to_rows(space_links)
    rows = t_rows.shape[-2]
    size = rows // n_lo * PACK
    f32 = jnp.float32
    dma = pltpu.SemaphoreType.DMA
    vmem = pl.BlockSpec(memory_space=pltpu.VMEM)
    some = lambda shape: jax.ShapeDtypeStruct(shape, f32)
    halo_shape = t_rows.shape[:3] + (max(steps - 1, 1),) + t_rows.shape[4:]
    packed_gauge, above, profile, mean, held_t, held_s = pl.pallas_call(
        functools.partial(scan_kernel, (steps, layers, n_gz, n_lo, n_hi)),
        out_shape=[
            some((14, rows, LANES)), some(t_rows.shape), some((steps, layers)),
            some((rows, LANES)), some(t_rows.shape), some(s_rows.shape),
        ],
        in_specs=[pl.BlockSpec(memory_space=pltpu.HBM)] * 2,
        out_specs=[vmem] * 6,
        scratch_shapes=[
            pltpu.VMEM(halo_shape, f32),
            pltpu.VMEM((2,) + s_rows.shape[1:], f32),
            pltpu.VMEM((rows * PACK, LANES), f32),
            pltpu.VMEM((n_lo, size, LANES), f32),
            pltpu.VMEM((size, LANES), f32),
            pltpu.VMEM((n_hi, size, LANES), f32),
            pltpu.VMEM((n_lo, size, LANES), f32),
            pltpu.VMEM((rows * PACK, LANES), f32),
            pltpu.VMEM((rows * PACK, LANES), f32),
            pltpu.VMEM((3, rows, LANES), f32),
            pltpu.VMEM((n_gz, rows, LANES), f32),
            pltpu.VMEM((n_lo, rows, LANES), f32),
            pltpu.VMEM((n_hi, rows, LANES), f32),
            dma((2,)),
            dma((n_lo,)), dma((n_lo,)), dma((n_hi,)), dma((n_hi,)), dma((n_lo,)), dma((n_lo,)),
            dma((n_lo,)), dma((n_lo,)), dma((2,)), dma((2,)),
            dma((n_gz,)), dma((n_gz,)), dma((n_lo,)), dma((n_lo,)), dma((n_hi,)), dma((n_hi,)),
        ],
        compiler_params=pltpu.CompilerParams(
            collective_id=0, has_side_effects=True, vmem_limit_bytes=GRANT
        ),
    )(*(pltpu.with_memory_space_constraint(a, pltpu.HBM) for a in (t_rows, s_rows)))
    gauge, fixed, profile, mean = pl.pallas_call(
        functools.partial(fix_kernel, (steps, layers)),
        out_shape=[some(t_rows.shape), some(s_rows.shape), some((steps, layers)), some((1, 1))],
        in_specs=[vmem] * 6,
        out_specs=[pl.BlockSpec(memory_space=pltpu.HBM)] * 4,
        scratch_shapes=[
            pltpu.VMEM(t_rows.shape, f32),
            pltpu.VMEM(s_rows.shape, f32),
            pltpu.VMEM((steps, layers), f32),
            pltpu.VMEM((1, 1), f32),
            dma((6,)),
        ],
        compiler_params=pltpu.CompilerParams(vmem_limit_bytes=GRANT),
    )(packed_gauge, above, profile, mean, held_t, held_s)
    return (
        from_rows(gauge, layers, sites),
        from_rows(fixed, layers, sites),
        profile,
        mean.reshape(()),
    )


def solution(mesh):
    return jax.shard_map(
        functools.partial(on_device, mesh.shape["ta"], mesh.shape["gz"]),
        mesh=mesh,
        in_specs=(
            P(None, None, None, "ta", "gz", None),
            P(None, None, None, None, "ta", "gz", None),
        ),
        out_specs=(
            P(None, None, None, "ta", "gz", None),
            P(None, None, None, None, "ta", "gz", None),
            P("ta", "gz"),
            P(),
        ),
        check_vma=False,
    )
```

```python
import functools

import jax
import jax.numpy as jnp
from jax import lax
from jax.experimental import pallas as pl
from jax.experimental.pallas import tpu as pltpu
from jax.sharding import PartitionSpec as P

X = 16
Y = 16
LANES = 128
GRANT = 8 << 20
MESH = pl.DeviceIdType.MESH
PACK = 16


def to_rows(a):
    lead, (z, s), n = a.shape[:-2], a.shape[-2:], a.ndim - 2
    a = jnp.swapaxes(a.reshape(lead + (z, s // LANES, LANES)), n, n + 1)
    return a.reshape(lead + (z * (s // LANES), LANES))


def from_rows(a, z, s):
    lead, n = a.shape[:-2], a.ndim - 2
    a = jnp.swapaxes(a.reshape(lead + (s // LANES, z, LANES)), n, n + 1)
    return a.reshape(lead + (z, s))


def product(a, b, rows=(0, 1, 2)):
    re, im = {}, {}
    for i in rows:
        for j in range(3):
            r = m = None
            for k in range(3):
                rr = a[0][i, k] * b[0][k, j] - a[1][i, k] * b[1][k, j]
                mm = a[0][i, k] * b[1][k, j] + a[1][i, k] * b[0][k, j]
                r = rr if r is None else r + rr
                m = mm if m is None else m + mm
            re[i, j], im[i, j] = r, m
    return re, im


def product_dagger(a, b):
    re, im = {}, {}
    for i in range(3):
        for j in range(3):
            r = m = None
            for k in range(3):
                rr = a[0][i, k] * b[0][j, k] + a[1][i, k] * b[1][j, k]
                mm = a[1][i, k] * b[0][j, k] - a[0][i, k] * b[1][j, k]
                r = rr if r is None else r + rr
                m = mm if m is None else m + mm
            re[i, j], im[i, j] = r, m
    return re, im


def cross_conj(m):
    re, im = m
    out_re, out_im = [], []
    for j in range(3):
        p, q = (j + 1) % 3, (j + 2) % 3
        out_re.append(
            (re[0, p] * re[1, q] - im[0, p] * im[1, q])
            - (re[0, q] * re[1, p] - im[0, q] * im[1, p])
        )
        out_im.append(
            (re[0, q] * im[1, p] + im[0, q] * re[1, p])
            - (re[0, p] * im[1, q] + im[0, p] * re[1, q])
        )
    return out_re, out_im


def determinant(m):
    wr, wi = cross_conj(m)
    re, im = m
    dr = sum(wr[j] * re[2, j] + wi[j] * im[2, j] for j in range(3))
    di = sum(wr[j] * im[2, j] - wi[j] * re[2, j] for j in range(3))
    return dr, di


def with_last_row(top, det):
    wr, wi = cross_conj(top)
    re, im = dict(top[0]), dict(top[1])
    for j in range(3):
        re[2, j] = det[0] * wr[j] - det[1] * wi[j]
        im[2, j] = det[0] * wi[j] + det[1] * wr[j]
    return re, im


TOP = [(i, j) for i in range(2) for j in range(3)]


def packed(top, det):
    return [top[0][e] for e in TOP] + [top[1][e] for e in TOP] + list(det)


def unpacked(v):
    top = ({e: v[n] for n, e in enumerate(TOP)}, {e: v[6 + n] for n, e in enumerate(TOP)})
    return top, (v[12], v[13])


def det_product(a, b):
    return a[0] * b[0] - a[1] * b[1], a[0] * b[1] + a[1] * b[0]


def put(ref, lead, count, values):
    for k, v in enumerate(values):
        ref[lead + (pl.ds(k, count, stride=PACK), slice(None))] = v


def get(ref, lead, count):
    return unpacked(
        [ref[lead + (pl.ds(k, count, stride=PACK), slice(None))] for k in range(14)]
    )


def matrix(ref, lead, t):
    re = {(i, j): ref[lead + (0, i, j, t)] for i in range(3) for j in range(3)}
    im = {(i, j): ref[lead + (1, i, j, t)] for i in range(3) for j in range(3)}
    return re, im


def keep(ref, lead, t, m):
    for i in range(3):
        for j in range(3):
            ref[lead + (0, i, j, t)] = m[0][i, j]
            ref[lead + (1, i, j, t)] = m[1][i, j]


def moved(f, *ms):
    return tuple({e: f(*(m[c][e] for m in ms)) for e in ms[0][c]} for c in range(2))


def steppers(rows, layers):
    lane = lax.broadcasted_iota(jnp.int32, (rows, LANES), 1)
    row = lax.broadcasted_iota(jnp.int32, (rows, LANES), 0)
    last_x = lane >= LANES - Y
    last_y = lane % Y == Y - 1
    last_z = row % layers == layers - 1

    def step_x(v):
        r = pltpu.roll(v, LANES - Y, 1)
        return jnp.where(last_x, pltpu.roll(r, rows - layers, 0), r)

    def step_y(v):
        return jnp.where(last_y, pltpu.roll(v, Y - 1, 1), pltpu.roll(v, LANES - 1, 1))

    def step_z(v, upper):
        return jnp.where(last_z, pltpu.roll(upper, layers - 1, 0), pltpu.roll(v, rows - 1, 0))

    return step_x, step_y, step_z, lane, row


def scan_kernel(
    sizes,
    time_in, space_in, gauge_out, above_out, profile_out, mean_out, tb, sb,
    halo_t, halo_s, pbuf, buf1, tot, buf2, obuf, gbuf, hbuf, msg, m1, m2, m3,
    in_sem, s1, r1, s2, r2, s3, r3, s4, r4, hs_sem, ht_sem, ms1, mr1, ms2, mr2, ms3, mr3,
    beside_sem, down_sem, up_sem,
):
    steps, layers, n_gz, n_lo, n_hi = sizes
    rows = tb.shape[-2]
    part = rows // n_lo
    size = part * PACK
    ta, gz = lax.axis_index("ta"), lax.axis_index("gz")
    hi, lo = ta // n_lo, ta % n_lo

    load_t = pltpu.make_async_copy(time_in, tb, in_sem.at[0])
    load_t.start()
    load_s = pltpu.make_async_copy(space_in, sb, in_sem.at[1])
    load_s.start()

    def flip(m):
        out, bit = 0, 1
        while bit < n_lo:
            b = (lo // bit) % 2
            out = out + bit * (1 - b if m & bit else b)
            bit *= 2
        return out

    def lo_at(m):
        return hi * n_lo + flip(m)

    def gz_at(d):
        return (gz + d) % n_gz

    def hi_at(d):
        return ((hi + d) % n_hi) * n_lo + lo

    barrier = pltpu.get_barrier_semaphore()
    for d in range(1, n_gz):
        pl.semaphore_signal(barrier, inc=1, device_id=(ta, gz_at(d)), device_id_type=MESH)
    for d in range(1, n_lo):
        pl.semaphore_signal(barrier, inc=1, device_id=(lo_at(d), gz), device_id_type=MESH)
    def tell(sem, device):
        pl.semaphore_signal(sem, inc=1, device_id=device, device_id_type=MESH)

    next_hi = ((ta + n_lo) % (n_hi * n_lo), gz)
    last_hi = ((ta + (n_hi - 1) * n_lo) % (n_hi * n_lo), gz)
    pl.when(hi < n_hi - 1)(lambda: tell(barrier, next_hi))
    pl.when(hi > 0)(lambda: tell(barrier, last_hi))

    def remote(src, dst, send, recv, device):
        return pltpu.make_async_remote_copy(
            src_ref=src, dst_ref=dst, send_sem=send, recv_sem=recv,
            device_id=device, device_id_type=MESH,
        )

    step_x, step_y, step_z, lane, row = steppers(rows, layers)

    load_t.wait()
    local = matrix(tb, (), 0)
    for t in range(1, steps):
        local = product(local, matrix(tb, (), t))
    put(pbuf, (), rows, packed(local, determinant(local)))

    ends = jnp.where(hi > 0, 1, 0) + jnp.where(hi < n_hi - 1, 1, 0)
    pl.semaphore_wait(barrier, n_gz - 1 + n_lo - 1 + ends)

    def mine(d):
        return pl.ds(pl.multiple_of(flip(d) * size, 8), size)

    far_first = sorted(range(1, n_lo), key=lambda m: -bin(m).count("1"))
    first = [pltpu.make_async_copy(pbuf.at[mine(0)], buf1.at[lo], s1.at[0])]
    for d in far_first:
        first.append(remote(pbuf.at[mine(d)], buf1.at[lo], s1.at[d], r1.at[d], (lo_at(d), gz)))
    for c in first[1:] + first[:1]:
        c.start()
    for d in range(1, n_lo):
        tell(beside_sem, (lo_at(d), gz))
    if n_hi > 2:
        pl.when(hi == n_hi - 2)(lambda: tell(down_sem, last_hi))
        pl.when(hi == 1)(lambda: tell(up_sem, next_hi))
    load_s.wait()
    below = gz_at(n_gz - 1)
    halo_link = remote(sb.at[pl.ds(0, 2)], halo_s, hs_sem.at[0], hs_sem.at[1], (ta, below))
    halo_link.start()
    halo_time = remote(
        tb.at[:, :, :, pl.ds(0, steps - 1)], halo_t, ht_sem.at[0], ht_sem.at[1], (ta, below)
    )
    if steps > 1:
        halo_time.start()

    def plaquette(a, b_moved, a_moved, b):
        u, v = product(a, b_moved), product(b, a_moved)
        re = sum(u[0][e] * v[0][e] + u[1][e] * v[1][e] for e in u[0])
        return 1.0 - re / 3.0

    density = []
    for t in range(steps):
        x, y = matrix(sb, (0,), t), matrix(sb, (1,), t)
        density.append(plaquette(x, moved(step_x, y), moved(step_y, x), y))
    if n_hi > 2:
        pl.when(hi <= n_hi - 3)(lambda: pl.semaphore_wait(down_sem, 1))
        pl.when((hi > 0) & (hi <= n_hi - 3))(lambda: tell(down_sem, last_hi))
        pl.when(hi >= 2)(lambda: pl.semaphore_wait(up_sem, 1))
        pl.when((hi < n_hi - 1) & (hi >= 2))(lambda: tell(up_sem, next_hi))
    halo_link.wait_recv()
    for t in range(steps):
        z = matrix(sb, (2,), t)
        for mu, step in ((0, step_x), (1, step_y)):
            a = matrix(sb, (mu,), t)
            up = moved(step_z, a, matrix(halo_s, (mu,), t))
            density[t] = density[t] + plaquette(a, moved(step, z), up, z)
    sites = rows // layers * LANES
    total = None
    for t in range(steps):
        per_row = jnp.broadcast_to(jnp.sum(density[t], axis=1, keepdims=True), (rows, LANES))
        spread = jnp.where(row % layers == lane, per_row, 0.0)
        line = jnp.sum(spread, axis=0, keepdims=True)
        profile_out[t : t + 1, :] = line[:, :layers] / float(sites) / 3.0
        total = per_row if total is None else total + per_row
    total = jnp.broadcast_to(jnp.sum(total, axis=0, keepdims=True), (rows, LANES))

    def spread_sum(n, stage, buf, me, send, recv, device, source):
        buf[me] = total_at[0]
        msg[stage] = total_at[0]
        out = [
            remote(msg.at[stage], buf.at[me], send.at[d], recv.at[d], device(d))
            for d in range(1, n)
        ]
        for c in out:
            c.start()
        return out

    def gather_sum(n, stage, buf, me, send, recv, device, source):
        for d in range(1, n):
            remote(
                msg.at[stage], buf.at[source(d)], send.at[d], recv.at[d], device(d)
            ).wait_recv()
        got = buf[0]
        for k in range(1, n):
            got = got + buf[k]
        total_at[0] = got

    total_at = [total]
    stage1 = (n_gz, 0, m1, gz, ms1, mr1, lambda d: (ta, gz_at(d)), lambda d: gz_at(n_gz - d))
    stage2 = (n_lo, 1, m2, lo, ms2, mr2, lambda d: (lo_at(d), gz), flip)
    stage3 = (n_hi, 2, m3, hi, ms3, mr3, lambda d: (hi_at(d), gz), lambda d: (hi + n_hi - d) % n_hi)
    sent = spread_sum(*stage1)

    first[0].wait()
    for d in range(1, n_lo):
        remote(
            pbuf.at[mine(d)], buf1.at[flip(d)], s1.at[d], r1.at[d], (lo_at(d), gz)
        ).wait_recv()
    before = [None]
    run, run_det = get(buf1, (0,), part)
    for k in range(1, n_lo):
        before.append((run, run_det))
        nxt, nxt_det = get(buf1, (k,), part)
        run = product(run, with_last_row(nxt, nxt_det), rows=(0, 1))
        run_det = det_product(run_det, nxt_det)
    put(tot, (), part, packed(run, run_det))

    def second(d, slot):
        return remote(tot, buf2.at[slot], s2.at[d], r2.at[d], (hi_at(d), gz))

    for d in reversed(range(1, n_hi)):
        pl.when(hi + d < n_hi)(second(d, hi).start)
    gather_sum(*stage1)
    sent += spread_sum(*stage2)
    gather_sum(*stage2)
    sent += spread_sum(*stage3)
    pl.semaphore_wait(beside_sem, n_lo - 1)
    full_before = [None] + [with_last_row(*b) for b in before[1:]]
    for d in range(1, n_hi):
        pl.when(hi >= d)(second(d, (hi + n_hi - d) % n_hi).wait_recv)

    zero = jnp.zeros((part, LANES), jnp.float32)
    one = jnp.ones((part, LANES), jnp.float32)
    acc = ({e: one if e[0] == e[1] else zero for e in TOP}, {e: zero for e in TOP})
    acc_det = (one, zero)
    for k in range(n_hi - 1):
        nxt, nxt_det = get(buf2, (k,), part)
        if k == 0:
            new, new_det = nxt, nxt_det
        else:
            new = product(acc, with_last_row(nxt, nxt_det), rows=(0, 1))
            new_det = det_product(acc_det, nxt_det)
        use = k < hi
        acc = moved(lambda n, o: jnp.where(use, n, o), new, acc)
        acc_det = tuple(jnp.where(use, n, o) for n, o in zip(new_det, acc_det))

    put(obuf, (0,), part, packed(acc, acc_det))
    for k in range(1, n_lo):
        top = product(acc, full_before[k], rows=(0, 1))
        put(obuf, (k,), part, packed(top, det_product(acc_det, before[k][1])))
    third = [pltpu.make_async_copy(obuf.at[lo], gbuf.at[mine(0)], s3.at[0])]
    for d in far_first:
        third.append(
            remote(obuf.at[flip(d)], gbuf.at[mine(0)], s3.at[d], r3.at[d], (lo_at(d), gz))
        )
    lowest = (lo * part) % layers == 0

    def fourth(d, source):
        rows_there = pl.ds(pl.multiple_of(source * size, 8), PACK)
        return remote(
            obuf.at[flip(d), pl.ds(0, PACK)], hbuf.at[rows_there], s4.at[d], r4.at[source],
            (lo_at(d), below),
        )

    for c in third[1:]:
        c.start()
    for d in far_first + [0]:
        pl.when(lowest)(fourth(d, lo).start)
    third[0].start()
    if steps > 1:
        halo_time.wait_recv()
    gather_sum(*stage3)
    count = sites * 3.0 * steps * layers * n_gz * n_lo * n_hi
    mean_out[...] = total_at[0] / count
    third[0].wait()
    for d in range(1, n_lo):
        remote(
            obuf.at[flip(d)], gbuf.at[mine(d)], s3.at[d], r3.at[d], (lo_at(d), gz)
        ).wait_recv()
    for k in range(14):
        gauge_out[k] = gbuf[pl.ds(k, rows, stride=PACK), :]
    for k in range(n_lo):
        if (k * part) % layers == 0:
            fourth(0, k).wait_recv()
    above = with_last_row(*get(hbuf, (), rows))
    for t in range(steps):
        keep(above_out, (), t, above)
        if t < steps - 1:
            above = product(above, matrix(halo_t, (), t))

    for c in first[1:] + third[1:] + sent + [halo_link]:
        c.wait_send()
    if steps > 1:
        halo_time.wait_send()
    for d in range(n_lo):
        pl.when(lowest)(fourth(d, lo).wait_send)
    for d in range(1, n_hi):
        pl.when(hi + d < n_hi)(second(d, hi).wait_send)


def fix_kernel(
    sizes,
    packed_in, above_in, profile_in, mean_in, tb, sb,
    gauge_out, fixed_out, profile_out, mean_out,
    gb, fb, pb, mb, out_sem,
):
    steps, layers = sizes
    rows = tb.shape[-2]
    pb[...] = profile_in[...]
    mb[...] = mean_in[0:1, 0:1]
    stores = [
        pltpu.make_async_copy(pb, profile_out, out_sem.at[4]),
        pltpu.make_async_copy(mb, mean_out, out_sem.at[5]),
    ]
    for c in stores:
        c.start()
    step_x, step_y, step_z, _, _ = steppers(rows, layers)
    gauge = with_last_row(*unpacked([packed_in[k] for k in range(14)]))
    for t in range(steps):
        keep(gb, (), t, gauge)
        if t < steps - 1:
            gauge = product(gauge, matrix(tb, (), t))
    stores.append(pltpu.make_async_copy(gb, gauge_out, out_sem.at[3]))
    stores[-1].start()
    for mu in range(3):
        for t in range(steps):
            g = matrix(gb, (), t)
            if mu == 2:
                ahead = moved(step_z, g, matrix(above_in, (), t))
            else:
                ahead = moved((step_x, step_y)[mu], g)
            keep(fb, (mu,), t, product_dagger(product(g, matrix(sb, (mu,), t)), ahead))
        stores.append(pltpu.make_async_copy(fb.at[mu], fixed_out.at[mu], out_sem.at[mu]))
        stores[-1].start()
    for c in stores:
        c.wait()


def on_device(n_ta, n_gz, time_links, space_links):
    steps, layers, sites = time_links.shape[3:]
    n_lo = 1
    while n_lo * 2 * n_lo * 2 <= n_ta:
        n_lo *= 2
    n_hi = n_ta // n_lo
    t_rows, s_rows = to_rows(time_links), to_rows(space_links)
    rows = t_rows.shape[-2]
    size = rows // n_lo * PACK
    f32 = jnp.float32
    dma, regular = pltpu.SemaphoreType.DMA, pltpu.SemaphoreType.REGULAR
    vmem = pl.BlockSpec(memory_space=pltpu.VMEM)
    some = lambda shape: jax.ShapeDtypeStruct(shape, f32)
    halo_shape = t_rows.shape[:3] + (max(steps - 1, 1),) + t_rows.shape[4:]
    packed_gauge, above, profile, mean, held_t, held_s = pl.pallas_call(
        functools.partial(scan_kernel, (steps, layers, n_gz, n_lo, n_hi)),
        out_shape=[
            some((14, rows, LANES)), some(t_rows.shape), some((steps, layers)),
            some((rows, LANES)), some(t_rows.shape), some(s_rows.shape),
        ],
        in_specs=[pl.BlockSpec(memory_space=pltpu.HBM)] * 2,
        out_specs=[vmem] * 6,
        scratch_shapes=[
            pltpu.VMEM(halo_shape, f32),
            pltpu.VMEM((2,) + s_rows.shape[1:], f32),
            pltpu.VMEM((rows * PACK, LANES), f32),
            pltpu.VMEM((n_lo, size, LANES), f32),
            pltpu.VMEM((size, LANES), f32),
            pltpu.VMEM((n_hi, size, LANES), f32),
            pltpu.VMEM((n_lo, size, LANES), f32),
            pltpu.VMEM((rows * PACK, LANES), f32),
            pltpu.VMEM((rows * PACK, LANES), f32),
            pltpu.VMEM((3, rows, LANES), f32),
            pltpu.VMEM((n_gz, rows, LANES), f32),
            pltpu.VMEM((n_lo, rows, LANES), f32),
            pltpu.VMEM((n_hi, rows, LANES), f32),
            dma((2,)),
            dma((n_lo,)), dma((n_lo,)), dma((n_hi,)), dma((n_hi,)), dma((n_lo,)), dma((n_lo,)),
            dma((n_lo,)), dma((n_lo,)), dma((2,)), dma((2,)),
            dma((n_gz,)), dma((n_gz,)), dma((n_lo,)), dma((n_lo,)), dma((n_hi,)), dma((n_hi,)),
            regular, regular, regular,
        ],
        compiler_params=pltpu.CompilerParams(
            collective_id=0, has_side_effects=True, vmem_limit_bytes=GRANT
        ),
    )(*(pltpu.with_memory_space_constraint(a, pltpu.HBM) for a in (t_rows, s_rows)))
    gauge, fixed, profile, mean = pl.pallas_call(
        functools.partial(fix_kernel, (steps, layers)),
        out_shape=[some(t_rows.shape), some(s_rows.shape), some((steps, layers)), some((1, 1))],
        in_specs=[vmem] * 6,
        out_specs=[pl.BlockSpec(memory_space=pltpu.HBM)] * 4,
        scratch_shapes=[
            pltpu.VMEM(t_rows.shape, f32),
            pltpu.VMEM(s_rows.shape, f32),
            pltpu.VMEM((steps, layers), f32),
            pltpu.VMEM((1, 1), f32),
            dma((6,)),
        ],
        compiler_params=pltpu.CompilerParams(vmem_limit_bytes=GRANT),
    )(packed_gauge, above, profile, mean, held_t, held_s)
    return (
        from_rows(gauge, layers, sites),
        from_rows(fixed, layers, sites),
        profile,
        mean.reshape(()),
    )


def solution(mesh):
    return jax.shard_map(
        functools.partial(on_device, mesh.shape["ta"], mesh.shape["gz"]),
        mesh=mesh,
        in_specs=(
            P(None, None, None, "ta", "gz", None),
            P(None, None, None, None, "ta", "gz", None),
        ),
        out_specs=(
            P(None, None, None, "ta", "gz", None),
            P(None, None, None, None, "ta", "gz", None),
            P("ta", "gz"),
            P(),
        ),
        check_vma=False,
    )
```
